32 devices in a mesh: fsdp: 8 (over z, x), tp: 4 (over y, core).
Axes of the slice: x: 2, y: 2, z: 4, core: 2. Of those that a mesh axis runs over, the one named last changes fastest.
Arguments:
- slopes_in: float32 [32, 128, 4096], P(None, 'fsdp', 'tp'), may hold values from -6 to 6
- moments_in: float32 [32, 128, 4096], P(None, 'fsdp', 'tp'), may hold values from -6 to 6
- weights_in: float32 [32, 128, 4096], P(None, 'fsdp', 'tp'), may hold values from -0.1875 to 0.1875
Outputs:
- new_weights: float32 [32, 128, 4096], P(None, 'fsdp', 'tp')
- new_momentum: float32 [32, 128, 4096], P(None, 'fsdp', 'tp')
The draws below stay inside these ranges and needn't reach their ends.
All inputs are finite; a program needn't handle non-finite values.
Results may differ from the reference program's by a relative error of at most 0.00021.
Values sent between devices are 32-bit elements; how exact they have to be, the bound alone decides.
A program may use at most 128 MiB of HBM per device.

```python
import jax
import jax.numpy as jnp
from jax import lax

SIDE = 128
WIDE = 4096
MATS = 32
ITERS = 5


def level_of(own_key, dims, split, smallest, top_value):
    level, own = 1.0, jax.random.fold_in(own_key, 6)
    for position, parts in split:
        heights = jnp.exp(jax.random.uniform(jax.random.fold_in(own, position), (parts,), jnp.float32, smallest / len(split), top_value / len(split)))
        level = level * jnp.repeat(heights, dims[position] // parts).reshape([-1 if axis == position else 1 for axis in range(len(dims))])
    return level


def normal_values(key, extent, scale, reach, cuts=(), held_as=jnp.bfloat16):
    loudness = level_of(key, extent, cuts, -0.22, 0.18) if cuts else 1.0
    array = jax.random.normal(key, extent, jnp.float32) * scale * loudness
    return jnp.minimum(jnp.maximum(array, -reach), reach).astype(held_as)


def setup_inputs(seed: int = 0) -> dict:
    seeds = jax.random.split(jax.random.key(seed), 4)
    slopes_in = normal_values(seeds[0], (MATS, SIDE, WIDE), 1.0, 6.0, ((1, 8), (2, 4)), jnp.float32)
    moments_in = normal_values(seeds[1], (MATS, SIDE, WIDE), 1.0, 6.0, ((1, 8), (2, 4)), jnp.float32)
    weights_in = normal_values(seeds[2], (MATS, SIDE, WIDE), 0.03, 0.1875, ((1, 8), (2, 4)), jnp.float32)
    return {"slopes_in": slopes_in, "moments_in": moments_in, "weights_in": weights_in}


hold_rate = 0.8
learn_rate = 1.0

def reference(slopes_in, moments_in, weights_in):
    new_momentum = hold_rate * moments_in + slopes_in

    def orthogonal_one(stack):
        iterate = stack[None]
        iterate = iterate * lax.rsqrt(lax.optimization_barrier(jnp.sum(iterate * iterate, axis=(1, 2), keepdims=True)) + 1e-06)
        for step in range(ITERS):
            gram = jnp.einsum('mik,mjk->mij', iterate, iterate, precision=lax.Precision.HIGHEST)
            mixed = -4.775 * gram + 2.0315 * jnp.einsum('mij,mjk->mik', gram, gram, precision=lax.Precision.HIGHEST)
            iterate = 3.4445 * iterate + jnp.einsum('mij,mjk->mik', mixed, iterate, precision=lax.Precision.HIGHEST)
        return iterate[0]
    iterate = lax.map(orthogonal_one, new_momentum)
    new_weights = weights_in - learn_rate * iterate
    return (new_weights, new_momentum)
```

```python
import functools

import jax
import jax.numpy as jnp
from jax import lax
from jax.sharding import PartitionSpec as P

ITERS = 5
HIGH = lax.Precision.HIGHEST


hold_rate = 0.8
learn_rate = 1.0


def polynomial(gram):
    side = gram.shape[-1]
    eye = jnp.eye(side, dtype=gram.dtype)
    dot = functools.partial(jnp.einsum, "mij,mjk->mik", precision=HIGH)
    scale = lax.rsqrt(jnp.sum(gram * eye, axis=(1, 2), keepdims=True) + 1e-06)
    gram = gram * (scale * scale)
    total = None
    for step in range(ITERS):
        mixed = 3.4445 * eye - 4.775 * gram + 2.0315 * dot(gram, gram)
        total = mixed * scale if total is None else dot(mixed, total)
        if step < ITERS - 1:
            gram = dot(dot(mixed, gram), mixed)
    return total


def body(slopes_in, moments_in, weights_in):
    new_momentum = hold_rate * moments_in + slopes_in
    moved = lax.all_to_all(new_momentum, "fsdp", split_axis=0, concat_axis=1, tiled=True)
    gram = lax.psum(jnp.einsum("mik,mjk->mij", moved, moved, precision=HIGH), "tp")
    iterate = jnp.einsum("mij,mjk->mik", polynomial(gram), moved, precision=HIGH)
    back = lax.all_to_all(iterate, "fsdp", split_axis=1, concat_axis=0, tiled=True)
    new_weights = weights_in - learn_rate * back
    return (new_weights, new_momentum)


def solution(mesh):
    return jax.shard_map(
        body,
        mesh=mesh,
        in_specs=(P(None, "fsdp", "tp"), P(None, "fsdp", "tp"), P(None, "fsdp", "tp")),
        out_specs=(P(None, "fsdp", "tp"), P(None, "fsdp", "tp")),
        check_vma=False,
    )
```

```python
import functools

import jax
import jax.numpy as jnp
from jax import lax
from jax.experimental import pallas as pl
from jax.experimental.pallas import tpu as pltpu
from jax.sharding import PartitionSpec as P

ITERS = 5
HIGH = lax.Precision.HIGHEST
MESH = pl.DeviceIdType.MESH


hold_rate = 0.8
learn_rate = 1.0


def polynomial(gram, dot, trace):
    side = gram.shape[-1]
    eye = jnp.where(
        lax.broadcasted_iota(jnp.int32, (side, side), 0) == lax.broadcasted_iota(jnp.int32, (side, side), 1), 1.0, 0.0
    ).astype(gram.dtype)
    scale = lax.rsqrt(trace(gram * eye) + 1e-06)
    gram = gram * (scale * scale)
    total = None
    for step in range(ITERS):
        mixed = 3.4445 * eye - 4.775 * gram + 2.0315 * dot(gram, gram)
        total = mixed * scale if total is None else dot(mixed, total)
        if step < ITERS - 1:
            gram = dot(dot(mixed, gram), mixed)
    return total


def kernel(stages, parts, cols, whole_ref, back_ref, x_ref, y_ref, g_ref, fsend, frecv, bsend, brecv, gsend, grecv, own):
    rows = whole_ref.shape[1]
    side, wide = parts * rows, whole_ref.shape[2]
    f, t = lax.axis_index("fsdp"), lax.axis_index("tp")
    hops = sorted(range(1, parts), key=lambda k: abs(2 * k - parts))

    barrier = pltpu.get_barrier_semaphore()
    for k in range(1, parts):
        pl.semaphore_signal(barrier, inc=1, device_id={"fsdp": lax.rem(f + k, parts)}, device_id_type=MESH)
    for k in range(1, cols):
        pl.semaphore_signal(barrier, inc=1, device_id={"tp": lax.rem(t + k, cols)}, device_id_type=MESH)
    pl.semaphore_wait(barrier, parts + cols - 2)

    def forward(m, peer, sender):
        return pltpu.make_async_remote_copy(
            src_ref=whole_ref.at[m * parts + peer], dst_ref=x_ref.at[m, sender],
            send_sem=fsend.at[m, peer], recv_sem=frecv.at[m, sender],
            device_id={"fsdp": peer}, device_id_type=MESH,
        )

    def backward(m, peer, sender):
        return pltpu.make_async_remote_copy(
            src_ref=y_ref.at[m, peer], dst_ref=back_ref.at[m * parts + sender],
            send_sem=bsend.at[m, peer], recv_sem=brecv.at[m, sender],
            device_id={"fsdp": peer}, device_id_type=MESH,
        )

    def partial(m, peer, sender):
        return pltpu.make_async_remote_copy(
            src_ref=g_ref.at[m, sender], dst_ref=g_ref.at[m, sender],
            send_sem=gsend.at[m, peer], recv_sem=grecv.at[m, sender],
            device_id={"tp": peer}, device_id_type=MESH,
        )

    def take(m):
        return pltpu.make_async_copy(whole_ref.at[m * parts + f], x_ref.at[m, f], own.at[0, m])

    def give(m):
        return pltpu.make_async_copy(y_ref.at[m, f], back_ref.at[m * parts + f], own.at[1, m])

    @pl.loop(0, stages)
    def _(m):
        for k in hops:
            forward(m, lax.rem(f + k, parts), f).start()
        take(m).start()

    dot = functools.partial(jnp.dot, precision=HIGH, preferred_element_type=jnp.float32)

    @pl.loop(0, stages)
    def _(m):
        take(m).wait()
        for k in hops:
            peer = lax.rem(f + k, parts)
            forward(m, peer, peer).wait_recv()
        x = x_ref[m].reshape(side, wide)
        g_ref[m, t] = lax.dot_general(x, x, (((1,), (1,)), ((), ())), precision=HIGH, preferred_element_type=jnp.float32)
        for k in range(1, cols):
            partial(m, lax.rem(t + k, cols), t).start()
        for k in range(1, cols):
            peer = lax.rem(t + k, cols)
            partial(m, peer, peer).wait_recv()
        gram = g_ref[m, 0]
        for k in range(1, cols):
            gram = gram + g_ref[m, k]
        total = polynomial(gram, dot, lambda a: jnp.sum(jnp.sum(a, axis=1, keepdims=True), axis=0, keepdims=True))
        y_ref[m] = dot(total, x_ref[m].reshape(side, wide)).reshape(parts, rows, wide)
        for k in hops:
            backward(m, lax.rem(f + k, parts), f).start()
        give(m).start()

    @pl.loop(0, stages)
    def _(m):
        give(m).wait()
        for k in hops:
            peer = lax.rem(f + k, parts)
            forward(m, peer, f).wait_send()
            backward(m, peer, f).wait_send()
            backward(m, peer, peer).wait_recv()
        for k in range(1, cols):
            partial(m, lax.rem(t + k, cols), t).wait_send()


def iterate_kernel(new_momentum, parts, cols):
    mats, rows, wide = new_momentum.shape
    stages, side = mats // parts, rows * parts
    dma = pltpu.SemaphoreType.DMA
    return pl.pallas_call(
        functools.partial(kernel, stages, parts, cols),
        out_shape=jax.ShapeDtypeStruct(new_momentum.shape, new_momentum.dtype),
        in_specs=[pl.BlockSpec(memory_space=pl.ANY)],
        out_specs=pl.BlockSpec(memory_space=pl.ANY),
        scratch_shapes=[
            pltpu.VMEM((stages, parts, rows, wide), jnp.float32),
            pltpu.VMEM((stages, parts, rows, wide), jnp.float32),
            pltpu.VMEM((stages, cols, side, side), jnp.float32),
            dma((stages, parts)), dma((stages, parts)), dma((stages, parts)), dma((stages, parts)),
            dma((stages, cols)), dma((stages, cols)), dma((2, stages)),
        ],
        compiler_params=pltpu.CompilerParams(collective_id=0, has_side_effects=True),
    )(new_momentum)


def iterate_plain(new_momentum):
    moved = lax.all_to_all(new_momentum, "fsdp", split_axis=0, concat_axis=1, tiled=True)
    gram = lax.psum(jnp.einsum("mik,mjk->mij", moved, moved, precision=HIGH), "tp")
    dot = functools.partial(jnp.einsum, "mij,mjk->mik", precision=HIGH)
    total = polynomial(gram, dot, lambda a: jnp.sum(a, axis=(1, 2), keepdims=True))
    return lax.all_to_all(dot(total, moved), "fsdp", split_axis=1, concat_axis=0, tiled=True)


def body(parts, cols, slopes_in, moments_in, weights_in):
    new_momentum = hold_rate * moments_in + slopes_in
    if new_momentum.shape[1] % 8 == 0:
        back = iterate_kernel(new_momentum, parts, cols)
    else:
        back = iterate_plain(new_momentum)
    new_weights = weights_in - learn_rate * back
    return (new_weights, new_momentum)


def solution(mesh):
    return jax.shard_map(
        functools.partial(body, mesh.shape["fsdp"], mesh.shape["tp"]),
        mesh=mesh,
        in_specs=(P(None, "fsdp", "tp"), P(None, "fsdp", "tp"), P(None, "fsdp", "tp")),
        out_specs=(P(None, "fsdp", "tp"), P(None, "fsdp", "tp")),
        check_vma=False,
    )
```

```python
import functools

import jax
import jax.numpy as jnp
from jax import lax
from jax.experimental import pallas as pl
from jax.experimental.pallas import tpu as pltpu
from jax.sharding import PartitionSpec as P

ITERS = 5
HIGH = lax.Precision.HIGHEST
MESH = pl.DeviceIdType.MESH


hold_rate = 0.8
learn_rate = 1.0


def polynomial(gram, dot, trace):
    side = gram.shape[-1]
    eye = jnp.where(
        lax.broadcasted_iota(jnp.int32, (side, side), 0) == lax.broadcasted_iota(jnp.int32, (side, side), 1), 1.0, 0.0
    ).astype(gram.dtype)
    scale = lax.rsqrt(trace(gram * eye) + 1e-06)
    gram = gram * (scale * scale)
    total = None
    for step in range(ITERS):
        mixed = 3.4445 * eye - 4.775 * gram + 2.0315 * dot(gram, gram)
        total = mixed * scale if total is None else dot(mixed, total)
        if step < ITERS - 1:
            gram = dot(dot(mixed, gram), mixed)
    return total


def kernel(
    stages, parts, cols, slopes_ref, moments_ref, weights_ref, momentum_ref, new_ref,
    s_ref, m_ref, w_ref, back_ref, whole_ref, x_ref, y_ref, g_ref, fsend, frecv, bsend, brecv, gsend, grecv, own, out,
):
    rows = whole_ref.shape[1]
    side, wide = parts * rows, whole_ref.shape[2]
    f, t = lax.axis_index("fsdp"), lax.axis_index("tp")
    hops = sorted(range(1, parts), key=lambda k: abs(2 * k - parts))

    def load(m, which, src, dst):
        some = pl.ds(m * parts, parts)
        return pltpu.make_async_copy(src.at[some], dst.at[some], own.at[which, m])

    @pl.loop(0, stages)
    def _(m):
        load(m, 2, slopes_ref, s_ref).start()
        load(m, 3, moments_ref, m_ref).start()

    barrier = pltpu.get_barrier_semaphore()
    for k in range(1, parts):
        pl.semaphore_signal(barrier, inc=1, device_id={"fsdp": lax.rem(f + parts + k * (1 - 2 * lax.rem(t, 2)), parts)}, device_id_type=MESH)
    for k in range(1, cols):
        pl.semaphore_signal(barrier, inc=1, device_id={"tp": lax.rem(t + k, cols)}, device_id_type=MESH)
    def forward(m, peer, sender):
        return pltpu.make_async_remote_copy(
            src_ref=whole_ref.at[m * parts + peer], dst_ref=x_ref.at[m, sender],
            send_sem=fsend.at[m, peer], recv_sem=frecv.at[m, sender],
            device_id={"fsdp": peer}, device_id_type=MESH,
        )

    def backward(m, peer, sender):
        return pltpu.make_async_remote_copy(
            src_ref=y_ref.at[m, peer], dst_ref=back_ref.at[m * parts + sender],
            send_sem=bsend.at[m, peer], recv_sem=brecv.at[m, sender],
            device_id={"fsdp": peer}, device_id_type=MESH,
        )

    def partial(m, peer, sender):
        return pltpu.make_async_remote_copy(
            src_ref=g_ref.at[m, sender], dst_ref=g_ref.at[m, sender],
            send_sem=gsend.at[m, peer], recv_sem=grecv.at[m, sender],
            device_id={"tp": peer}, device_id_type=MESH,
        )

    def take(m):
        return pltpu.make_async_copy(whole_ref.at[m * parts + f], x_ref.at[m, f], own.at[5, m])

    def give(m):
        return pltpu.make_async_copy(y_ref.at[m, f], back_ref.at[m * parts + f], own.at[1, m])

    def put(m, peer):
        mat = m * parts + peer
        return pltpu.make_async_copy(w_ref.at[mat], new_ref.at[mat], out.at[m, peer])

    def finish(m, peer):
        mat = m * parts + peer
        w_ref[mat] = w_ref[mat] - learn_rate * back_ref[mat]
        put(m, peer).start()

    def add(m):
        load(m, 2, slopes_ref, s_ref).wait()
        load(m, 3, moments_ref, m_ref).wait()
        some = pl.ds(m * parts, parts)
        whole_ref[some] = hold_rate * m_ref[some] + s_ref[some]

    add(0)
    pl.semaphore_wait(barrier, parts + cols - 2)

    @pl.loop(0, stages)
    def _(m):
        @pl.when(m > 0)
        def _():
            add(m)

        for k in hops:
            forward(m, lax.rem(f + parts + k * (1 - 2 * lax.rem(t, 2)), parts), f).start()
        take(m).start()
        load(m, 4, whole_ref, momentum_ref).start()
        load(m, 0, weights_ref, w_ref).start()

    dot = functools.partial(jnp.dot, precision=HIGH, preferred_element_type=jnp.float32)

    @pl.loop(0, stages)
    def _(m):
        take(m).wait()
        for k in hops:
            peer = lax.rem(f + parts + k * (1 - 2 * lax.rem(t, 2)), parts)
            forward(m, peer, peer).wait_recv()
        x = x_ref[m].reshape(side, wide)
        g_ref[m, t] = lax.dot_general(x, x, (((1,), (1,)), ((), ())), precision=HIGH, preferred_element_type=jnp.float32)
        for k in range(1, cols):
            partial(m, lax.rem(t + k, cols), t).start()
        for k in range(1, cols):
            peer = lax.rem(t + k, cols)
            partial(m, peer, peer).wait_recv()
        gram = g_ref[m, 0]
        for k in range(1, cols):
            gram = gram + g_ref[m, k]
        total = polynomial(gram, dot, lambda a: jnp.sum(jnp.sum(a, axis=1, keepdims=True), axis=0, keepdims=True))
        y_ref[m] = dot(total, x_ref[m].reshape(side, wide)).reshape(parts, rows, wide)
        for k in hops:
            backward(m, lax.rem(f + parts + k * (1 - 2 * lax.rem(t, 2)), parts), f).start()
        give(m).start()

    @pl.loop(0, stages)
    def _(m):
        give(m).wait()
        load(m, 0, weights_ref, w_ref).wait()
        finish(m, f)
        for k in hops:
            peer = lax.rem(f + parts + k * (1 - 2 * lax.rem(t, 2)), parts)
            backward(m, peer, peer).wait_recv()
            finish(m, peer)

    @pl.loop(0, stages)
    def _(m):
        load(m, 4, whole_ref, momentum_ref).wait()
        put(m, f).wait()
        for k in hops:
            peer = lax.rem(f + parts + k * (1 - 2 * lax.rem(t, 2)), parts)
            put(m, peer).wait()
            forward(m, peer, f).wait_send()
            backward(m, peer, f).wait_send()
        for k in range(1, cols):
            partial(m, lax.rem(t + k, cols), t).wait_send()


def leave(first_ref, second_ref, first_out, second_out, sems):
    copies = [pltpu.make_async_copy(first_ref, first_out, sems.at[0]), pltpu.make_async_copy(second_ref, second_out, sems.at[1])]
    for copy in copies:
        copy.start()
    for copy in copies:
        copy.wait()


def leave_kernel(first, second):
    return pl.pallas_call(
        leave,
        out_shape=[jax.ShapeDtypeStruct(a.shape, a.dtype) for a in (first, second)],
        in_specs=[pl.BlockSpec(memory_space=pl.ANY)] * 2,
        out_specs=[pl.BlockSpec(memory_space=pl.ANY)] * 2,
        scratch_shapes=[pltpu.SemaphoreType.DMA((2,))],
        compiler_params=pltpu.CompilerParams(vmem_limit_bytes=2**20),
    )(first, second)


def iterate_kernel(slopes_in, moments_in, weights_in, parts, cols):
    mats, rows, wide = slopes_in.shape
    stages, side = mats // parts, rows * parts
    dma = pltpu.SemaphoreType.DMA
    return pl.pallas_call(
        functools.partial(kernel, stages, parts, cols),
        out_shape=[jax.ShapeDtypeStruct(slopes_in.shape, slopes_in.dtype)] * 2,
        in_specs=[pl.BlockSpec(memory_space=pltpu.HBM)] * 3,
        out_specs=[pl.BlockSpec(memory_space=pl.ANY)] * 2,
        scratch_shapes=[
            *[pltpu.VMEM((mats, rows, wide), jnp.float32)] * 5,
            pltpu.VMEM((stages, parts, rows, wide), jnp.float32),
            pltpu.VMEM((stages, parts, rows, wide), jnp.float32),
            pltpu.VMEM((stages, cols, side, side), jnp.float32),
            dma((stages, parts)), dma((stages, parts)), dma((stages, parts)), dma((stages, parts)),
            dma((stages, cols)), dma((stages, cols)), dma((6, stages)), dma((stages, parts)),
        ],
        compiler_params=pltpu.CompilerParams(collective_id=0, has_side_effects=True, vmem_limit_bytes=48 * 2**20),
    )(slopes_in, moments_in, weights_in)


def iterate_plain(new_momentum):
    moved = lax.all_to_all(new_momentum, "fsdp", split_axis=0, concat_axis=1, tiled=True)
    gram = lax.psum(jnp.einsum("mik,mjk->mij", moved, moved, precision=HIGH), "tp")
    dot = functools.partial(jnp.einsum, "mij,mjk->mik", precision=HIGH)
    total = polynomial(gram, dot, lambda a: jnp.sum(a, axis=(1, 2), keepdims=True))
    return lax.all_to_all(dot(total, moved), "fsdp", split_axis=1, concat_axis=0, tiled=True)


def body(parts, cols, slopes_in, moments_in, weights_in):
    if slopes_in.shape[1] % 8 == 0:
        new_momentum, new_weights = iterate_kernel(slopes_in, moments_in, weights_in, parts, cols)
        new_weights, new_momentum = leave_kernel(new_weights, new_momentum)
    else:
        new_momentum = hold_rate * moments_in + slopes_in
        new_weights = weights_in - learn_rate * iterate_plain(new_momentum)
    return (new_weights, new_momentum)


def solution(mesh):
    return jax.shard_map(
        functools.partial(body, mesh.shape["fsdp"], mesh.shape["tp"]),
        mesh=mesh,
        in_specs=(P(None, "fsdp", "tp"), P(None, "fsdp", "tp"), P(None, "fsdp", "tp")),
        out_specs=(P(None, "fsdp", "tp"), P(None, "fsdp", "tp")),
        check_vma=False,
    )
```
